128 devices in a mesh: section: 4 (over x_lo, core), rep: 32 (over x_hi, z, y).
Axes of the slice: x: 4 (x_hi: 2, x_lo: 2; x = x_hi * 2 + x_lo), y: 4, z: 4, core: 2. Of those that a mesh axis runs over, the one named last changes fastest.
Arguments:
- x_in: bfloat16 [32, 768, 1024], P('rep'), may hold values from -6 to 6
- cotangent: bfloat16 [32, 768, 1024], P('rep'), may hold values from -6 to 6
- norm_gain: float32 [4, 1024], P('section'), may hold values from 0.1 to 1.9
- w_up: bfloat16 [32, 4, 1024, 2048], P('rep', 'section'), may hold values from -0.1875 to 0.1875
- w_down: bfloat16 [32, 4, 2048, 1024], P('rep', 'section'), may hold values from -0.125 to 0.125
- live: int32 [32], replicated, may hold values from 0 to 1, as said below
- donor: int32 [32], replicated, may hold values from 0 to 31, as said below
Outputs:
- section_out: bfloat16 [32, 4, 768, 1024], P('rep', 'section')
- section_in_grad: bfloat16 [32, 4, 768, 1024], P('rep', 'section')
- grad_up: bfloat16 [32, 4, 1024, 2048], P('rep', 'section')
- grad_down: bfloat16 [32, 4, 2048, 1024], P('rep', 'section')
The draws below stay inside these ranges and needn't reach their ends.
Inputs may be any that keep to these rules, and one draw needn't show every extreme that they name: At least one replica is dead and at least half are live. `donor`: for a dead replica, the index of a live replica; for a live replica any index, unused.
All inputs are finite; a program needn't handle non-finite values.
Results may differ from the reference program's by a relative error of at most 0.014.
Values may be sent and summed in bfloat16 or wider, within the bound.
No kernel may reach another device: no remote copies, remote signals or barrier semaphores. Data moves between devices by JAX's collectives and lax.ppermute only.
A program may use at most 320 MiB of HBM per device.

```python
import jax
import jax.numpy as jnp
from jax import lax

D = 1024
F = 2048
TOK = 768
REPLICAS = 32
SECTIONS = 4


def exploit_maps(key):
    base = jax.random.fold_in(key, 7)
    order = jax.random.permutation(jax.random.fold_in(base, 1), REPLICAS)
    dead_count = jax.random.randint(jax.random.fold_in(base, 2), (), 1, REPLICAS // 2 + 1)
    ranks = jnp.argsort(order)
    alive = (ranks >= dead_count).astype(jnp.int32)
    picks = jax.random.randint(jax.random.fold_in(base, 3), (REPLICAS,), 0, REPLICAS - dead_count)
    chosen = order[(dead_count + picks).astype(jnp.int32)].astype(jnp.int32)
    others = jax.random.randint(jax.random.fold_in(base, 4), (REPLICAS,), 0, REPLICAS)
    donors = jnp.where(alive == 1, others, chosen).astype(jnp.int32)
    return (alive, donors)


def draw_live(key, part):
    alive, donors = exploit_maps(key)
    return alive


def draw_donor(key, part):
    alive, donors = exploit_maps(key)
    return donors


def block_scale(own_key, dims, split, least, top_value):
    def one(position, parts):
        heights = jax.random.uniform(jax.random.fold_in(jax.random.fold_in(own_key, 6), position), (parts,), jnp.float32, least / len(split), top_value / len(split))
        return jnp.repeat(jnp.exp(heights), dims[position] // parts).reshape((-1,) + (1,) * (len(dims) - position - 1))

    loudness = one(*split[0])
    for cut in split[1:]:
        loudness = loudness * one(*cut)
    return loudness


def centred(key, extent, deviation, limit, cuts=(), held_as=jnp.bfloat16):
    array = jax.random.normal(key, extent, jnp.float32) * deviation
    if len(cuts) > 0:
        array = block_scale(key, extent, cuts, -0.22, 0.18) * array
    return jnp.clip(array, min=-limit, max=limit).astype(held_as)


def setup_inputs(seed: int = 0) -> dict:
    keys = jax.random.split(jax.random.key(seed), 8)
    return {
        "x_in": centred(keys[0], (REPLICAS, TOK, D), 1.0, 6.0, ((0, 32),)),
        "cotangent": centred(keys[1], (REPLICAS, TOK, D), 1.0, 6.0, ((0, 32),)),
        "norm_gain": jnp.clip(1.0 + 0.18 * jax.random.normal(keys[2], (SECTIONS, D), jnp.float32), 0.1, 1.9),
        "w_up": centred(keys[3], (REPLICAS, SECTIONS, D, F), D ** -0.5, 0.1875, ((0, 32), (1, 4))),
        "w_down": centred(keys[4], (REPLICAS, SECTIONS, F, D), F ** -0.5, 0.125, ((0, 32), (1, 4))),
        "live": draw_live(jax.random.fold_in(keys[7], 71), 0),
        "donor": draw_donor(jax.random.fold_in(keys[7], 71), 0),
    }


GELU_C = 0.7978845608028654

def gelu_value(u):
    inner = jnp.tanh(GELU_C * (u + 0.044715 * u * u * u))
    return 0.5 * u * (1.0 + inner)

def gelu_slope(u):
    inner = jnp.tanh(GELU_C * (u + 0.044715 * u * u * u))
    return 0.5 * (1.0 + inner) + 0.5 * u * (1.0 - inner * inner) * GELU_C * (1.0 + 3.0 * 0.044715 * u * u)

def contract(left, right, left_dim, right_dim):
    return lax.dot_general(left, right, (((left_dim,), (right_dim,)), ((), ())), preferred_element_type=jnp.float32)

def norm_components(token_rows):
    values = token_rows.astype(jnp.float32)
    center = values - lax.optimization_barrier(jnp.mean(values, axis=-1, keepdims=True))
    scale_factor = lax.rsqrt(lax.optimization_barrier(jnp.mean(center * center, axis=-1, keepdims=True)) + 1e-05)
    return (center * scale_factor, scale_factor)

def layer_forward(token_rows, gain_vector, up_proj, down_proj):
    standardized_input, scale_factor = norm_components(token_rows)
    normalized_rows = (standardized_input * gain_vector).astype(jnp.bfloat16)
    pre = contract(normalized_rows, up_proj, 1, 0)
    hidden = gelu_value(pre).astype(jnp.bfloat16)
    out = (token_rows.astype(jnp.float32) + contract(hidden, down_proj, 1, 0)).astype(jnp.bfloat16)
    return (normalized_rows, pre, hidden, out)

def layer_backward(token_rows, grad_out, gain_vector, up_proj, down_proj, normalized_rows, pre, hidden):
    grad_hidden = contract(grad_out, down_proj, 1, 1)
    grad_pre = (grad_hidden * gelu_slope(pre)).astype(jnp.bfloat16)
    step_up = contract(normalized_rows, grad_pre, 0, 0)
    step_down = contract(hidden, grad_out, 0, 0)
    grad_normed = contract(grad_pre, up_proj, 1, 1)
    standardized_input, scale_factor = norm_components(token_rows)
    weighted_rows = grad_normed * gain_vector
    centered_rows = weighted_rows - lax.optimization_barrier(jnp.mean(weighted_rows, axis=-1, keepdims=True)) - standardized_input * lax.optimization_barrier(jnp.mean(weighted_rows * standardized_input, axis=-1, keepdims=True))
    grad_in = (grad_out.astype(jnp.float32) + scale_factor * centered_rows).astype(jnp.bfloat16)
    return (grad_in, step_up, step_down)

def reference(x_in, cotangent, norm_gain, w_up, w_down, live, donor):

    def one_replica(index):
        alive = live[index] == 1
        source = donor[index]
        ups = jnp.where(alive, w_up[index], w_up[source])
        downs = jnp.where(alive, w_down[index], w_down[source])
        token_rows = x_in[index]
        inputs, kept, outputs = ([], [], [])
        for level in range(SECTIONS):
            normalized_rows, pre, hidden, out = layer_forward(token_rows, norm_gain[level], ups[level], downs[level])
            inputs.append(token_rows)
            kept.append((normalized_rows, pre, hidden))
            outputs.append(out)
            token_rows = out
        grad_out = cotangent[index]
        grads_in, grads_up, grads_down = ([None] * SECTIONS, [None] * SECTIONS, [None] * SECTIONS)
        for level in range(SECTIONS - 1, -1, -1):
            normalized_rows, pre, hidden = kept[level]
            grad_in, step_up, step_down = layer_backward(inputs[level], grad_out, norm_gain[level], ups[level], downs[level], normalized_rows, pre, hidden)
            grads_in[level] = grad_in
            grads_up[level] = step_up.astype(jnp.bfloat16)
            grads_down[level] = step_down.astype(jnp.bfloat16)
            grad_out = grad_in
        return (jnp.stack(outputs), jnp.stack(grads_in), jnp.stack(grads_up), jnp.stack(grads_down))
    section_out, section_in_grad, grad_up, grad_down = lax.map(one_replica, jnp.arange(REPLICAS, dtype=jnp.int32))
    return (section_out, section_in_grad, grad_up, grad_down)
```

```python
import functools

import jax
import jax.numpy as jnp
from jax import lax
from jax.experimental import pallas as pl
from jax.experimental.pallas import tpu as pltpu
from jax.sharding import PartitionSpec as P

MICRO = 4
CHUNK = 512
LAG_FAST = 2
LAG_SLOW = 3
GELU_C = 0.7978845608028654
VMEM_LIMIT = 40 * 1024 * 1024


def row_stats(values):
    center = values - jnp.mean(values, axis=-1, keepdims=True)
    factor = lax.rsqrt(jnp.mean(center * center, axis=-1, keepdims=True) + 1e-05)
    return center * factor, factor


def mm(left, right, left_dim, right_dim):
    return lax.dot_general(
        left, right, (((left_dim,), (right_dim,)), ((), ())), preferred_element_type=jnp.float32
    )


def choose(level, sources):
    value = sources[-1][1][...]
    for levels, ref in sources[:-1]:
        hit = functools.reduce(jnp.logical_or, [level == k for k in levels])
        value = jnp.where(hit, ref[...], value)
    return value


def forward_body(levels_of, meta, *refs):
    n_src = len(levels_of)
    sources = list(zip(levels_of, refs[:n_src]))
    gain, up, down = refs[n_src : n_src + 3]
    send, rows_out, normed_out, hidden_out, slope_out, out = refs[n_src + 8 : n_src + 14]
    normed_s, acc = refs[n_src + 14 :]
    step = pl.program_id(0)
    last = pl.num_programs(0) - 1

    @pl.when(meta[1] == 1)
    def _():
        @pl.when(step == 0)
        def _():
            rows = choose(meta[2], sources)
            rows_out[...] = rows
            xhat, _ = row_stats(rows.astype(jnp.float32))
            normed = (xhat * gain[...]).astype(jnp.bfloat16)
            normed_s[...] = normed
            normed_out[...] = normed
            acc[...] = rows.astype(jnp.float32)

        u = mm(normed_s[...], up[...], 1, 0)
        inner = jnp.tanh(GELU_C * (u + 0.044715 * u * u * u))
        half = 0.5 * (1.0 + inner)
        hidden = (u * half).astype(jnp.bfloat16)
        slope = half + 0.5 * u * (1.0 - inner * inner) * GELU_C * (1.0 + 3.0 * 0.044715 * u * u)
        hidden_out[...] = hidden
        slope_out[...] = slope.astype(jnp.bfloat16)
        acc[...] += mm(hidden, down[...], 1, 0)

        @pl.when(step == last)
        def _():
            result = acc[...].astype(jnp.bfloat16)
            send[...] = result
            out[...] = result


def backward_body(levels_of, meta, *refs):
    n_src = len(levels_of)
    sources = list(zip(levels_of, refs[:n_src]))
    gain, up, down, rows, slope = refs[n_src : n_src + 5]
    send, grad_out, pre_out, grad_in = refs[n_src + 8 : n_src + 12]
    grad_s, acc = refs[n_src + 12 :]
    step = pl.program_id(0)
    last = pl.num_programs(0) - 1

    @pl.when(meta[1] == 1)
    def _():
        @pl.when(step == 0)
        def _():
            grad = choose(meta[2], sources)
            grad_s[...] = grad
            grad_out[...] = grad
            acc[...] = jnp.zeros_like(acc)

        grad_hidden = mm(grad_s[...], down[...], 1, 1)
        grad_pre = (grad_hidden * slope[...].astype(jnp.float32)).astype(jnp.bfloat16)
        pre_out[...] = grad_pre
        acc[...] += mm(grad_pre, up[...], 1, 1)

        @pl.when(step == last)
        def _():
            xhat, factor = row_stats(rows[...].astype(jnp.float32))
            q = acc[...] * gain[...]
            centered = (
                q
                - jnp.mean(q, axis=-1, keepdims=True)
                - xhat * jnp.mean(q * xhat, axis=-1, keepdims=True)
            )
            result = (grad_s[...].astype(jnp.float32) + factor * centered).astype(jnp.bfloat16)
            send[...] = result
            grad_in[...] = result


def source_spec(kind, m, width):
    if kind == "slot":
        return pl.BlockSpec((m, width), lambda j, meta: (jnp.minimum(meta[0], MICRO - 1), 0))
    return pl.BlockSpec((m, width), lambda j, meta: (0, 0))


def stage(body, name, meta, sources, weights, reads, stash, m, flops):
    gain, up, down = weights
    width, hidden = up.shape
    steps = hidden // CHUNK

    def live(j, meta):
        return jnp.where(meta[1] == 1, j, 0)

    def slot_spec(array):
        if array.shape[1] == hidden:
            return pl.BlockSpec((m, CHUNK), lambda j, meta: (meta[0], j))
        return pl.BlockSpec((m, width), lambda j, meta: (meta[0], 0))

    def read_spec(array):
        if array.shape[1] == hidden:
            return pl.BlockSpec((m, CHUNK), lambda j, meta: (meta[0], live(j, meta)))
        return pl.BlockSpec((m, width), lambda j, meta: (meta[0], 0))

    in_specs = [source_spec(kind, m, width) for _, kind, _ in sources]
    in_specs += [
        pl.BlockSpec((1, width), lambda j, meta: (0, 0)),
        pl.BlockSpec((width, CHUNK), lambda j, meta: (0, live(j, meta))),
        pl.BlockSpec((CHUNK, width), lambda j, meta: (live(j, meta), 0)),
    ]
    in_specs += [read_spec(a) for a in reads]
    n_before = len(in_specs)
    in_specs += [pl.BlockSpec(memory_space=pl.ANY) for _ in stash]
    out_specs = [pl.BlockSpec((m, width), lambda j, meta: (0, 0))]
    out_specs += [slot_spec(a) for a in stash]
    outs = [jax.ShapeDtypeStruct((m, width), jnp.bfloat16)]
    outs += [jax.ShapeDtypeStruct(a.shape, a.dtype) for a in stash]
    call = pl.pallas_call(
        functools.partial(body, [levels for levels, _, _ in sources]),
        grid_spec=pltpu.PrefetchScalarGridSpec(
            num_scalar_prefetch=1,
            grid=(steps,),
            in_specs=in_specs,
            out_specs=out_specs,
            scratch_shapes=[
                pltpu.VMEM((m, width), jnp.bfloat16),
                pltpu.VMEM((m, width), jnp.float32),
            ],
        ),
        out_shape=outs,
        input_output_aliases={1 + n_before + i: 1 + i for i in range(len(stash))},
        compiler_params=pltpu.CompilerParams(
            dimension_semantics=("arbitrary",), vmem_limit_bytes=VMEM_LIMIT
        ),
        cost_estimate=pl.CostEstimate(
            flops=flops, bytes_accessed=2 * 2 * width * hidden, transcendentals=0
        ),
        name=name,
    )
    result = call(meta, *[a for _, _, a in sources], gain, up, down, *reads, *stash)
    return result[0], list(result[1:])


def relay(body, name, entry, offsets, direction, level, weights, reads, stash, m):
    depth = len(offsets)
    width, hidden = weights[1].shape
    flops = 4 * m * width * hidden
    rounds = max(offsets) + MICRO
    sent = {}
    head = 0 if direction > 0 else depth - 1
    table = jnp.asarray(offsets, jnp.int32)
    offset = table[level]
    for turn in range(rounds):
        active = [s for s in range(depth) if 0 <= turn - offsets[s] < MICRO]
        index = turn - offset
        valid = (index >= 0) & (index < MICRO)
        slot = jnp.where(valid, index, MICRO)
        meta = jnp.stack([slot, valid.astype(jnp.int32), level]).astype(jnp.int32)
        by_array = {}
        for s in active:
            key = None if s == head else (s - direction, turn - (offsets[s] - offsets[s - direction]))
            array_key = "entry" if key is None else sent[key][0]
            by_array.setdefault(array_key, []).append(s)
        sources = []
        for array_key, levels in by_array.items():
            if array_key == "entry":
                sources.append((levels, "slot", entry))
            else:
                sources.append((levels, "whole", arrays[array_key]))
        send, stash = stage(body, name, meta, sources, weights, reads, stash, m, flops)
        groups = {}
        for s in active:
            if 0 <= s + direction < depth:
                lag = offsets[s + direction] - offsets[s]
                groups.setdefault(lag, []).append(s)
        for lag, members in groups.items():
            moved = lax.ppermute(send, "section", [(s, s + direction) for s in members])
            if turn == 0:
                arrays = {}
            arrays[(turn, lag)] = moved
            for s in members:
                sent[(s, turn)] = ((turn, lag),)
    return stash


def per_device(x_in, cotangent, norm_gain, w_up, w_down, live, donor):
    member = lax.axis_index("rep")
    level = lax.axis_index("section")
    depth = lax.axis_size("section")
    peers = lax.axis_size("rep")
    own_up = w_up[0, 0]
    own_down = w_down[0, 0]
    width, hidden_width = own_up.shape
    tokens = x_in.shape[1]
    m = tokens // MICRO

    def spread(own):
        return lax.all_to_all(
            own.reshape(peers, -1, own.shape[1]), "rep", split_axis=0, concat_axis=0, tiled=True
        )

    def collect(pieces):
        picked = pieces.at[donor].get(mode="promise_in_bounds")
        back = lax.all_to_all(picked, "rep", split_axis=0, concat_axis=0, tiled=True)
        return back.reshape(-1, back.shape[-1])

    alive = live[member] == 1
    held_up = spread(own_up)
    held_down = spread(own_down)
    used_up = jnp.where(alive, own_up, collect(held_up))
    used_down = jnp.where(alive, own_down, collect(held_down))
    weights = (norm_gain, used_up, used_down)

    def space(columns):
        return jnp.zeros(((MICRO + 1) * m, columns), jnp.bfloat16)

    lags = [LAG_SLOW if s % 2 else LAG_FAST for s in range(depth - 1)]
    offsets = [sum(lags[:s]) for s in range(depth)]
    rows, normed, hidden, slope, outs = relay(
        forward_body, "section_forward", x_in[0], offsets, 1, level, weights, [],
        [space(width), space(width), space(hidden_width), space(hidden_width), space(width)], m,
    )
    grads, pres, grads_in = relay(
        backward_body, "section_backward", cotangent[0], offsets[::-1], -1, level, weights,
        [rows, slope], [space(width), space(hidden_width), space(width)], m,
    )
    grad_up = mm(normed[:tokens], pres[:tokens], 0, 0).astype(jnp.bfloat16)
    grad_down = mm(hidden[:tokens], grads[:tokens], 0, 0).astype(jnp.bfloat16)
    return (
        outs[:tokens][None, None],
        grads_in[:tokens][None, None],
        grad_up[None, None],
        grad_down[None, None],
    )


def solution(mesh):
    return jax.shard_map(
        per_device,
        mesh=mesh,
        in_specs=(
            P("rep", None, None),
            P("rep", None, None),
            P("section", None),
            P("rep", "section", None, None),
            P("rep", "section", None, None),
            P(),
            P(),
        ),
        out_specs=(
            P("rep", "section", None, None),
            P("rep", "section", None, None),
            P("rep", "section", None, None),
            P("rep", "section", None, None),
        ),
        check_vma=False,
    )
```

```python
import functools

import jax
import jax.numpy as jnp
from jax import lax
from jax.experimental import pallas as pl
from jax.experimental.pallas import tpu as pltpu
from jax.sharding import PartitionSpec as P

MICRO = 4
CHUNK = 512
LAG_FAST = 2
LAG_SLOW = 3
GELU_C = 0.7978845608028654
VMEM_LIMIT = 24 * 1024 * 1024


def row_stats(values):
    center = values - jnp.mean(values, axis=-1, keepdims=True)
    factor = lax.rsqrt(jnp.mean(center * center, axis=-1, keepdims=True) + 1e-05)
    return center * factor, factor


def mm(left, right, left_dim, right_dim):
    return lax.dot_general(
        left, right, (((left_dim,), (right_dim,)), ((), ())), preferred_element_type=jnp.float32
    )


def choose(level, sources):
    value = sources[-1][1][...]
    for levels, ref in sources[:-1]:
        hit = functools.reduce(jnp.logical_or, [level == k for k in levels])
        value = jnp.where(hit, ref[...], value)
    return value


def forward_body(levels_of, n_stash, meta, *refs):
    n_src = len(levels_of)
    sources = list(zip(levels_of, refs[:n_src]))
    gain, up, down = refs[n_src : n_src + 3]
    refs = refs[n_src + 3 + n_stash :]
    send, rows_h, normed_h, hidden_h, slope_h, out_h = refs[:6]
    rows_s, normed_s, hidden_s, slope_s, sems = refs[6:]
    m, hidden_width = hidden_s.shape
    place = pl.ds(pl.multiple_of(meta[0] * m, m), m)

    def store(k, source, target):
        return pltpu.make_async_copy(source, target.at[place, :], sems.at[k])

    @pl.when(meta[1] == 1)
    def _():
        rows = choose(meta[2], sources)
        rows_s[...] = rows
        xhat, _ = row_stats(rows.astype(jnp.float32))
        normed_s[...] = (xhat * gain[...]).astype(jnp.bfloat16)
        store(0, rows_s, rows_h).start()
        store(1, normed_s, normed_h).start()
        for j in range(hidden_width // CHUNK):
            cut = slice(j * CHUNK, (j + 1) * CHUNK)
            u = mm(normed_s[...], up[:, cut], 1, 0)
            inner = jnp.tanh(GELU_C * (u + 0.044715 * u * u * u))
            half = 0.5 * (1.0 + inner)
            hidden_s[:, cut] = (u * half).astype(jnp.bfloat16)
            slope_s[:, cut] = (
                half + 0.5 * u * (1.0 - inner * inner) * GELU_C * (1.0 + 3.0 * 0.044715 * u * u)
            ).astype(jnp.bfloat16)
        store(2, hidden_s, hidden_h).start()
        store(3, slope_s, slope_h).start()
        total = rows_s[...].astype(jnp.float32) + mm(hidden_s[...], down[...], 1, 0)
        send[...] = total.astype(jnp.bfloat16)
        store(4, send, out_h).start()
        for k, (source, target) in enumerate(
            [(rows_s, rows_h), (normed_s, normed_h), (hidden_s, hidden_h), (slope_s, slope_h), (send, out_h)]
        ):
            store(k, source, target).wait()


def backward_body(levels_of, n_stash, meta, *refs):
    n_src = len(levels_of)
    sources = list(zip(levels_of, refs[:n_src]))
    gain, up, down, rows_h, slope_h = refs[n_src : n_src + 5]
    refs = refs[n_src + 5 + n_stash :]
    send, grad_h, pre_h, grad_in_h = refs[:4]
    grad_s, rows_s, slope_s, pre_s, sems = refs[4:]
    m, hidden_width = pre_s.shape
    place = pl.ds(pl.multiple_of(meta[0] * m, m), m)

    def store(k, source, target):
        return pltpu.make_async_copy(source, target.at[place, :], sems.at[k])

    def load(k, source, target):
        return pltpu.make_async_copy(source.at[place, :], target, sems.at[k])

    @pl.when(meta[1] == 1)
    def _():
        load(0, slope_h, slope_s).start()
        load(1, rows_h, rows_s).start()
        grad_s[...] = choose(meta[2], sources)
        store(2, grad_s, grad_h).start()
        load(0, slope_h, slope_s).wait()
        for j in range(hidden_width // CHUNK):
            cut = slice(j * CHUNK, (j + 1) * CHUNK)
            grad_hidden = mm(grad_s[...], down[cut, :], 1, 1)
            pre_s[:, cut] = (grad_hidden * slope_s[:, cut].astype(jnp.float32)).astype(jnp.bfloat16)
        store(3, pre_s, pre_h).start()
        load(1, rows_h, rows_s).wait()
        q = mm(pre_s[...], up[...], 1, 1) * gain[...]
        xhat, factor = row_stats(rows_s[...].astype(jnp.float32))
        centered = (
            q
            - jnp.mean(q, axis=-1, keepdims=True)
            - xhat * jnp.mean(q * xhat, axis=-1, keepdims=True)
        )
        send[...] = (grad_s[...].astype(jnp.float32) + factor * centered).astype(jnp.bfloat16)
        store(4, send, grad_in_h).start()
        store(2, grad_s, grad_h).wait()
        store(3, pre_s, pre_h).wait()
        store(4, send, grad_in_h).wait()


def stage(body, name, meta, sources, weights, reads, stash, shapes, m, flops, scratch):
    gain, up, down = weights
    width, hidden = up.shape
    whole = pl.BlockSpec(memory_space=pltpu.VMEM)
    far = pl.BlockSpec(memory_space=pltpu.HBM)
    in_specs = []
    for _, kind, _ in sources:
        if kind == "slot":
            in_specs.append(
                pl.BlockSpec((m, width), lambda j, meta: (jnp.minimum(meta[0], MICRO - 1), 0))
            )
        else:
            in_specs.append(pl.BlockSpec((m, width), lambda j, meta: (0, 0)))
    in_specs += [whole] * 3 + [far] * len(reads)
    n_before = len(in_specs)
    held = stash or []
    in_specs += [far] * len(held)
    out_specs = [pl.BlockSpec((m, width), lambda j, meta: (0, 0))] + [far] * len(shapes)
    outs = [jax.ShapeDtypeStruct((m, width), jnp.bfloat16)]
    outs += [jax.ShapeDtypeStruct(s, jnp.bfloat16) for s in shapes]
    call = pl.pallas_call(
        functools.partial(body, [levels for levels, _, _ in sources], len(held)),
        grid_spec=pltpu.PrefetchScalarGridSpec(
            num_scalar_prefetch=1,
            grid=(1,),
            in_specs=in_specs,
            out_specs=out_specs,
            scratch_shapes=scratch + [pltpu.SemaphoreType.DMA((5,))],
        ),
        out_shape=outs,
        input_output_aliases={1 + n_before + i: 1 + i for i in range(len(held))},
        compiler_params=pltpu.CompilerParams(
            dimension_semantics=("arbitrary",), vmem_limit_bytes=VMEM_LIMIT
        ),
        cost_estimate=pl.CostEstimate(
            flops=flops, bytes_accessed=2 * 2 * width * hidden, transcendentals=0
        ),
        name=name,
    )
    result = call(meta, *[a for _, _, a in sources], gain, up, down, *reads, *held)
    return result[0], list(result[1:])


def relay(body, name, entry, offsets, direction, level, weights, reads, columns, m, scratch):
    depth = len(offsets)
    width, hidden = weights[1].shape
    flops = 4 * m * width * hidden
    shapes = [(MICRO * m, c) for c in columns]
    rounds = max(offsets) + MICRO
    head = 0 if direction > 0 else depth - 1
    offset = jnp.asarray(offsets, jnp.int32)[level]
    arrays = {}
    stash = None
    for turn in range(rounds):
        active = [s for s in range(depth) if 0 <= turn - offsets[s] < MICRO]
        index = turn - offset
        valid = (index >= 0) & (index < MICRO)
        slot = jnp.clip(index, 0, MICRO - 1)
        meta = jnp.stack([slot, valid.astype(jnp.int32), level]).astype(jnp.int32)
        by_array = {}
        for s in active:
            lag = None if s == head else offsets[s] - offsets[s - direction]
            by_array.setdefault(lag, []).append(s)
        sources = [
            (levels, "slot", entry) if lag is None else (levels, "whole", arrays[turn - lag, lag])
            for lag, levels in by_array.items()
        ]
        send, stash = stage(body, name, meta, sources, weights, reads, stash, shapes, m, flops, scratch)
        groups = {}
        for s in active:
            if 0 <= s + direction < depth:
                groups.setdefault(offsets[s + direction] - offsets[s], []).append(s)
        for lag, members in groups.items():
            arrays[turn, lag] = lax.ppermute(send, "section", [(s, s + direction) for s in members])
    return stash


def per_device(x_in, cotangent, norm_gain, w_up, w_down, live, donor):
    member = lax.axis_index("rep")
    level = lax.axis_index("section")
    depth = lax.axis_size("section")
    peers = lax.axis_size("rep")
    own_up = w_up[0, 0]
    own_down = w_down[0, 0]
    width, hidden_width = own_up.shape
    tokens = x_in.shape[1]
    m = tokens // MICRO

    def spread(own):
        return lax.all_to_all(
            own.reshape(peers, -1, own.shape[1]), "rep", split_axis=0, concat_axis=0, tiled=True
        )

    def collect(pieces):
        picked = pieces.at[donor].get(mode="promise_in_bounds")
        back = lax.all_to_all(picked, "rep", split_axis=0, concat_axis=0, tiled=True)
        return back.reshape(-1, back.shape[-1])

    alive = live[member] == 1
    held_up = spread(own_up)
    held_down = spread(own_down)
    used_up = jnp.where(alive, own_up, collect(held_up))
    used_down = jnp.where(alive, own_down, collect(held_down))
    weights = (norm_gain, used_up, used_down)
    lags = [LAG_SLOW if s % 2 else LAG_FAST for s in range(depth - 1)]
    offsets = [sum(lags[:s]) for s in range(depth)]

    def rows_of(columns):
        return pltpu.VMEM((m, columns), jnp.bfloat16)

    rows, normed, hidden, slope, outs = relay(
        forward_body, "section_forward", x_in[0], offsets, 1, level, weights, [],
        [width, width, hidden_width, hidden_width, width], m,
        [rows_of(width), rows_of(width), rows_of(hidden_width), rows_of(hidden_width)],
    )
    grads, pres, grads_in = relay(
        backward_body, "section_backward", cotangent[0], offsets[::-1], -1, level, weights,
        [rows, slope], [width, hidden_width, width], m,
        [rows_of(width), rows_of(width), rows_of(hidden_width), rows_of(hidden_width)],
    )
    grad_up = mm(normed, pres, 0, 0).astype(jnp.bfloat16)
    grad_down = mm(hidden, grads, 0, 0).astype(jnp.bfloat16)
    return (outs[None, None], grads_in[None, None], grad_up[None, None], grad_down[None, None])


def solution(mesh):
    return jax.shard_map(
        per_device,
        mesh=mesh,
        in_specs=(
            P("rep", None, None),
            P("rep", None, None),
            P("section", None),
            P("rep", "section", None, None),
            P("rep", "section", None, None),
            P(),
            P(),
        ),
        out_specs=(
            P("rep", "section", None, None),
            P("rep", "section", None, None),
            P("rep", "section", None, None),
            P("rep", "section", None, None),
        ),
        check_vma=False,
    )
```

```python
import functools

import jax
import jax.numpy as jnp
from jax import lax
from jax.experimental import pallas as pl
from jax.experimental.pallas import tpu as pltpu
from jax.sharding import PartitionSpec as P

MICRO = 4
CHUNK = 512
LAG_FAST = 2
LAG_SLOW = 3
GELU_C = 0.7978845608028654
CUBIC = 0.044715
VMEM_LIMIT = 16 * 1024 * 1024
COPY_LIMIT = 62 * 1024 * 1024
SETTLE_LIMIT = 44 * 1024 * 1024
VMEM = pl.BlockSpec(memory_space=pltpu.VMEM)
SMEM = pl.BlockSpec(memory_space=pltpu.SMEM)
FAR = pl.BlockSpec(memory_space=pl.ANY)


def row_stats(values):
    center = values - jnp.mean(values, axis=-1, keepdims=True)
    factor = lax.rsqrt(jnp.mean(center * center, axis=-1, keepdims=True) + 1e-05)
    return center * factor, factor


def mm(left, right, left_dim, right_dim):
    return lax.dot_general(
        left, right, (((left_dim,), (right_dim,)), ((), ())), preferred_element_type=jnp.float32
    )


def gelu_and_slope(u):
    square = u * u
    half = 0.5 + 0.5 * jnp.tanh(u * (GELU_C + (GELU_C * CUBIC) * square))
    slope = half + (half - half * half) * (
        u * (2.0 * GELU_C + (6.0 * GELU_C * CUBIC) * square)
    )
    return u * half, slope


def choose(level, place, sources):
    def read(kind, ref):
        return ref[place, :] if kind == "slot" else ref[...]

    value = read(*sources[-1][1:])
    for levels, kind, ref in sources[:-1]:
        hit = functools.reduce(jnp.logical_or, [level == k for k in levels])
        value = jnp.where(hit, read(kind, ref), value)
    return value


def forward_body(heads, n_held, m, meta, *refs):
    sources = [(*head, ref) for head, ref in zip(heads, refs)]
    gain, up, down = refs[len(heads) : len(heads) + 3]
    send, rows_o, normed_o, hidden_o, slope_o, out_o, sem = refs[len(heads) + 3 + n_held :]
    place = pl.ds(pl.multiple_of(meta[0] * m, m), m)

    @pl.when(meta[1] == 1)
    def _():
        rows = choose(meta[2], place, sources)
        rows_o[place, :] = rows
        xhat, _ = row_stats(rows.astype(jnp.float32))
        normed = (xhat * gain[...]).astype(jnp.bfloat16)
        normed_o[place, :] = normed
        for j in range(up.shape[1] // CHUNK):
            cut = slice(j * CHUNK, (j + 1) * CHUNK)
            hidden, slope = gelu_and_slope(mm(normed, up[:, cut], 1, 0))
            hidden_o[place, cut] = hidden.astype(jnp.bfloat16)
            slope_o[place, cut] = slope.astype(jnp.bfloat16)
        for j in range(down.shape[1] // CHUNK):
            cut = slice(j * CHUNK, (j + 1) * CHUNK)
            total = rows_o[place, cut].astype(jnp.float32) + mm(
                hidden_o[place, :], down[:, cut], 1, 0
            )
            send[:, cut] = total.astype(jnp.bfloat16)
        keep = pltpu.make_async_copy(send, out_o.at[place, :], sem)
        keep.start()
        keep.wait()


def backward_body(heads, n_held, m, meta, *refs):
    sources = [(*head, ref) for head, ref in zip(heads, refs)]
    gain, up, down, rows_i, slope_i = refs[len(heads) : len(heads) + 5]
    send, grad_o, pre_o, grad_in_o, sem = refs[len(heads) + 5 + n_held :]
    place = pl.ds(pl.multiple_of(meta[0] * m, m), m)

    @pl.when(meta[1] == 1)
    def _():
        grad = choose(meta[2], place, sources)
        grad_o[place, :] = grad
        for j in range(up.shape[1] // CHUNK):
            cut = slice(j * CHUNK, (j + 1) * CHUNK)
            grad_hidden = mm(grad, down[cut, :], 1, 1)
            pre_o[place, cut] = (grad_hidden * slope_i[place, cut].astype(jnp.float32)).astype(
                jnp.bfloat16
            )
        q = mm(pre_o[place, :], up[...], 1, 1) * gain[...]
        xhat, factor = row_stats(rows_i[place, :].astype(jnp.float32))
        centered = (
            q
            - jnp.mean(q, axis=-1, keepdims=True)
            - xhat * jnp.mean(q * xhat, axis=-1, keepdims=True)
        )
        result = (grad.astype(jnp.float32) + factor * centered).astype(jnp.bfloat16)
        send[...] = result
        keep = pltpu.make_async_copy(send, grad_in_o.at[place, :], sem)
        keep.start()
        keep.wait()


def stage(body, name, meta, sources, weights, reads, held, shapes, m):
    width, hidden = weights[1].shape
    operands = [a for _, _, a in sources] + list(weights) + list(reads) + list(held)
    n_before = len(operands) - len(held)
    result = pl.pallas_call(
        functools.partial(body, [s[:2] for s in sources], len(held), m),
        in_specs=[SMEM] + [VMEM] * n_before + ([VMEM] * (len(held) - 1) + [FAR] if held else []),
        out_specs=[VMEM] * len(shapes) + [FAR],
        out_shape=[jax.ShapeDtypeStruct(s, jnp.bfloat16) for s in [(m, width)] + shapes],
        scratch_shapes=[pltpu.SemaphoreType.DMA],
        input_output_aliases={1 + n_before + i: 1 + i for i in range(len(held))},
        compiler_params=pltpu.CompilerParams(vmem_limit_bytes=VMEM_LIMIT),
        cost_estimate=pl.CostEstimate(
            flops=4 * m * width * hidden, bytes_accessed=4 * width * hidden, transcendentals=0
        ),
        name=name,
    )(meta, *operands)
    return result[0], list(result[1:])


def relay(body, name, entry, offsets, direction, level, weights, reads, columns, m):
    depth = len(offsets)
    shapes = [(MICRO * m, c) for c in columns]
    head = 0 if direction > 0 else depth - 1
    offset = jnp.asarray(offsets, jnp.int32)[level]
    arrays = {}
    held = []
    for turn in range(max(offsets) + MICRO):
        active = [s for s in range(depth) if 0 <= turn - offsets[s] < MICRO]
        index = turn - offset
        valid = (index >= 0) & (index < MICRO)
        slot = jnp.clip(index, 0, MICRO - 1)
        meta = jnp.stack([slot, valid.astype(jnp.int32), level]).astype(jnp.int32)
        by_array = {}
        for s in active:
            lag = None if s == head else offsets[s] - offsets[s - direction]
            by_array.setdefault(lag, []).append(s)
        sources = [
            (levels, "slot", entry) if lag is None else (levels, "whole", arrays[turn - lag, lag])
            for lag, levels in by_array.items()
        ]
        send, held = stage(body, name, meta, sources, weights, reads, held, shapes, m)
        groups = {}
        for s in active:
            if 0 <= s + direction < depth:
                groups.setdefault(offsets[s + direction] - offsets[s], []).append(s)
        for lag, members in groups.items():
            arrays[turn, lag] = lax.ppermute(send, "section", [(s, s + direction) for s in members])
    return held


def pick_body(live, donor, held, picked, room, in_sems, out_sems):
    def load(j):
        return pltpu.make_async_copy(held.at[donor[j]], room.at[j], in_sems.at[j])

    def save(j):
        return pltpu.make_async_copy(room.at[j], picked.at[j], out_sems.at[j])

    def each(action):
        def step(j, carry):
            @pl.when(live[j] == 0)
            def _():
                action(j)

            return carry

        lax.fori_loop(0, held.shape[0], step, 0)

    def pass_on(j):
        load(j).wait()
        save(j).start()

    each(lambda j: load(j).start())
    each(pass_on)
    each(lambda j: save(j).wait())


def pick(held, live, donor):
    peers = held.shape[0]
    return pl.pallas_call(
        pick_body,
        in_specs=[SMEM, SMEM, FAR],
        out_specs=FAR,
        out_shape=jax.ShapeDtypeStruct(held.shape, held.dtype),
        scratch_shapes=[
            pltpu.VMEM(held.shape, held.dtype),
            pltpu.SemaphoreType.DMA((peers,)),
            pltpu.SemaphoreType.DMA((peers,)),
        ],
        compiler_params=pltpu.CompilerParams(vmem_limit_bytes=COPY_LIMIT),
        cost_estimate=pl.CostEstimate(flops=1 << 32, bytes_accessed=1 << 23, transcendentals=0),
        name="pick_pieces",
    )(live, donor, held)


def settle_body(alive, arrived, own, used, sem):
    def run(source):
        copy = pltpu.make_async_copy(source, used, sem)
        copy.start()
        copy.wait()

    @pl.when(alive[0] == 1)
    def _():
        run(own)

    @pl.when(alive[0] == 0)
    def _():
        run(arrived)


def settle(alive, arrived, own):
    return pl.pallas_call(
        settle_body,
        in_specs=[SMEM, FAR, FAR],
        out_specs=VMEM,
        out_shape=jax.ShapeDtypeStruct(own.shape, own.dtype),
        scratch_shapes=[pltpu.SemaphoreType.DMA],
        compiler_params=pltpu.CompilerParams(vmem_limit_bytes=SETTLE_LIMIT),
        cost_estimate=pl.CostEstimate(flops=1 << 31, bytes_accessed=1 << 22, transcendentals=0),
        name="settle_weights",
    )(alive, arrived, own)


def per_device(x_in, cotangent, norm_gain, w_up, w_down, live, donor):
    member = lax.axis_index("rep")
    level = lax.axis_index("section")
    depth = lax.axis_size("section")
    peers = lax.axis_size("rep")
    own_up = w_up[0, 0]
    own_down = w_down[0, 0]
    width, hidden_width = own_up.shape
    tokens = x_in.shape[1]
    m = tokens // MICRO

    def exchange(pieces):
        return lax.all_to_all(pieces, "rep", split_axis=0, concat_axis=0, tiled=True)

    alive = lax.dynamic_slice_in_dim(live, member, 1)

    def share(own):
        held = exchange(own.reshape(peers, -1, own.shape[1]))
        arrived = exchange(pick(held, live, donor))
        return settle(alive, arrived.reshape(own.shape), own)

    weights = (norm_gain, share(own_up), share(own_down))
    lags = [LAG_SLOW if s % 2 else LAG_FAST for s in range(depth - 1)]
    offsets = [sum(lags[:s]) for s in range(depth)]
    rows, normed, hidden, slope, outs = relay(
        forward_body, "section_forward", x_in[0], offsets, 1, level, weights, [],
        [width, width, hidden_width, hidden_width, width], m,
    )
    grads, pres, grads_in = relay(
        backward_body, "section_backward", cotangent[0], offsets[::-1], -1, level, weights,
        [rows, slope], [width, hidden_width, width], m,
    )
    grad_up = mm(normed, pres, 0, 0).astype(jnp.bfloat16)
    grad_down = mm(hidden, grads, 0, 0).astype(jnp.bfloat16)
    return (outs[None, None], grads_in[None, None], grad_up[None, None], grad_down[None, None])


def solution(mesh):
    return jax.shard_map(
        per_device,
        mesh=mesh,
        in_specs=(
            P("rep", None, None),
            P("rep", None, None),
            P("section", None),
            P("rep", "section", None, None),
            P("rep", "section", None, None),
            P(),
            P(),
        ),
        out_specs=(
            P("rep", "section", None, None),
            P("rep", "section", None, None),
            P("rep", "section", None, None),
            P("rep", "section", None, None),
        ),
        check_vma=False,
    )
```

```python
import functools

import jax
import jax.numpy as jnp
from jax import lax
from jax.experimental import pallas as pl
from jax.experimental.pallas import tpu as pltpu
from jax.sharding import PartitionSpec as P

MICRO = 3
CHUNK = 512
LAG_FAST = 1
LAG_SLOW = 2
GELU_C = 0.7978845608028654
CUBIC = 0.044715
VMEM_LIMIT = 16 * 1024 * 1024
COPY_LIMIT = 62 * 1024 * 1024
SETTLE_LIMIT = 44 * 1024 * 1024
VMEM = pl.BlockSpec(memory_space=pltpu.VMEM)
SMEM = pl.BlockSpec(memory_space=pltpu.SMEM)
FAR = pl.BlockSpec(memory_space=pl.ANY)


def row_stats(values):
    center = values - jnp.mean(values, axis=-1, keepdims=True)
    factor = lax.rsqrt(jnp.mean(center * center, axis=-1, keepdims=True) + 1e-05)
    return center * factor, factor


def mm(left, right, left_dim, right_dim):
    return lax.dot_general(
        left, right, (((left_dim,), (right_dim,)), ((), ())), preferred_element_type=jnp.float32
    )


def gelu_and_slope(u):
    square = u * u
    half = 0.5 + 0.5 * jnp.tanh(u * (GELU_C + (GELU_C * CUBIC) * square))
    slope = half + (half - half * half) * (
        u * (2.0 * GELU_C + (6.0 * GELU_C * CUBIC) * square)
    )
    return u * half, slope


def choose(level, place, sources):
    def read(kind, ref):
        return ref[place, :] if kind == "slot" else ref[...]

    value = read(*sources[-1][1:])
    for levels, kind, ref in sources[:-1]:
        hit = functools.reduce(jnp.logical_or, [level == k for k in levels])
        value = jnp.where(hit, read(kind, ref), value)
    return value


def forward_body(heads, n_held, m, meta, *refs):
    sources = [(*head, ref) for head, ref in zip(heads, refs)]
    gain, up, down = refs[len(heads) : len(heads) + 3]
    send, rows_o, slope_o, normed_o, hidden_o, out_o = refs[len(heads) + 3 + n_held :]
    place = pl.ds(pl.multiple_of(meta[0] * m, m), m)

    @pl.when(meta[1] == 1)
    def _():
        rows = choose(meta[2], place, sources)
        rows_o[place, :] = rows
        xhat, _ = row_stats(rows.astype(jnp.float32))
        normed = (xhat * gain[...]).astype(jnp.bfloat16)
        normed_o[place, :] = normed
        for j in range(up.shape[1] // CHUNK):
            cut = slice(j * CHUNK, (j + 1) * CHUNK)
            hidden, slope = gelu_and_slope(mm(normed, up[:, cut], 1, 0))
            hidden_o[place, cut] = hidden.astype(jnp.bfloat16)
            slope_o[place, cut] = slope.astype(jnp.bfloat16)
        for j in range(down.shape[1] // CHUNK):
            cut = slice(j * CHUNK, (j + 1) * CHUNK)
            total = rows_o[place, cut].astype(jnp.float32) + mm(
                hidden_o[place, :], down[:, cut], 1, 0
            )
            send[:, cut] = total.astype(jnp.bfloat16)
            out_o[place, cut] = send[:, cut]


def backward_body(heads, n_held, m, meta, *refs):
    sources = [(*head, ref) for head, ref in zip(heads, refs)]
    gain, up, down = refs[len(heads) : len(heads) + 3]
    send, rows_i, slope_i, grad_o, pre_o, grad_in_o = refs[len(heads) + 3 + n_held :]
    place = pl.ds(pl.multiple_of(meta[0] * m, m), m)

    @pl.when(meta[1] == 1)
    def _():
        grad = choose(meta[2], place, sources)
        grad_o[place, :] = grad
        for j in range(up.shape[1] // CHUNK):
            cut = slice(j * CHUNK, (j + 1) * CHUNK)
            grad_hidden = mm(grad, down[cut, :], 1, 1)
            pre_o[place, cut] = (grad_hidden * slope_i[place, cut].astype(jnp.float32)).astype(
                jnp.bfloat16
            )
        q = mm(pre_o[place, :], up[...], 1, 1) * gain[...]
        xhat, factor = row_stats(rows_i[place, :].astype(jnp.float32))
        centered = (
            q
            - jnp.mean(q, axis=-1, keepdims=True)
            - xhat * jnp.mean(q * xhat, axis=-1, keepdims=True)
        )
        result = (grad.astype(jnp.float32) + factor * centered).astype(jnp.bfloat16)
        send[...] = result
        grad_in_o[place, :] = result


def stage(body, name, meta, sources, weights, held, shapes, m):
    width, hidden = weights[1].shape
    given = [i for i, a in enumerate(held) if a is not None]
    operands = [a for _, _, a in sources] + list(weights)
    n_before = len(operands)
    operands += [held[i] for i in given]
    result = pl.pallas_call(
        functools.partial(body, [s[:2] for s in sources], len(given), m),
        in_specs=[SMEM] + [VMEM] * n_before + [VMEM] * len(given),
        out_specs=[VMEM] * (1 + len(shapes)),
        out_shape=[jax.ShapeDtypeStruct(s, jnp.bfloat16) for s in [(m, width)] + shapes],
        input_output_aliases={1 + n_before + k: 1 + i for k, i in enumerate(given)},
        compiler_params=pltpu.CompilerParams(vmem_limit_bytes=VMEM_LIMIT),
        cost_estimate=pl.CostEstimate(
            flops=4 * m * width * hidden, bytes_accessed=4 * width * hidden, transcendentals=0
        ),
        name=name,
    )(meta, *operands)
    return result[0], list(result[1:])


class Relay:
    def __init__(self, body, name, entry, offsets, direction, level, weights, m):
        self.body, self.name, self.entry = body, name, entry
        self.offsets, self.direction, self.level = offsets, direction, level
        self.weights, self.m = weights, m
        self.arrays = {}

    def active(self, turn):
        return [s for s, o in enumerate(self.offsets) if 0 <= turn - o < MICRO]

    def run(self, turn, held, shapes):
        offsets, direction = self.offsets, self.direction
        depth = len(offsets)
        head = 0 if direction > 0 else depth - 1
        active = self.active(turn)
        index = turn - jnp.asarray(offsets, jnp.int32)[self.level]
        valid = (index >= 0) & (index < MICRO)
        slot = jnp.clip(index, 0, MICRO - 1)
        meta = jnp.stack([slot, valid.astype(jnp.int32), self.level]).astype(jnp.int32)
        by_array = {}
        for s in active:
            lag = None if s == head else offsets[s] - offsets[s - direction]
            by_array.setdefault(lag, []).append(s)
        sources = [
            (levels, "slot", self.entry)
            if lag is None
            else (levels, "whole", self.arrays[turn - lag, lag])
            for lag, levels in by_array.items()
        ]
        send, held = stage(
            self.body, self.name, meta, sources, self.weights, held, shapes, self.m
        )
        groups = {}
        for s in active:
            if 0 <= s + direction < depth:
                groups.setdefault(offsets[s + direction] - offsets[s], []).append(s)
        for lag, members in groups.items():
            pairs = [(s, s + direction) for s in members]
            self.arrays[turn, lag] = lax.ppermute(send, "section", pairs)
        return held


def pick_body(live, donor, held, picked, room, in_sems, out_sems):
    def load(j):
        return pltpu.make_async_copy(held.at[donor[j]], room.at[j], in_sems.at[j])

    def save(j):
        return pltpu.make_async_copy(room.at[j], picked.at[j], out_sems.at[j])

    def each(action):
        def step(j, carry):
            @pl.when(live[j] == 0)
            def _():
                action(j)

            return carry

        lax.fori_loop(0, held.shape[0], step, 0)

    def pass_on(j):
        load(j).wait()
        save(j).start()

    each(lambda j: load(j).start())
    each(pass_on)
    each(lambda j: save(j).wait())


def pick(held, live, donor):
    peers = held.shape[0]
    return pl.pallas_call(
        pick_body,
        in_specs=[SMEM, SMEM, FAR],
        out_specs=FAR,
        out_shape=jax.ShapeDtypeStruct(held.shape, held.dtype),
        scratch_shapes=[
            pltpu.VMEM(held.shape, held.dtype),
            pltpu.SemaphoreType.DMA((peers,)),
            pltpu.SemaphoreType.DMA((peers,)),
        ],
        compiler_params=pltpu.CompilerParams(vmem_limit_bytes=COPY_LIMIT),
        cost_estimate=pl.CostEstimate(flops=1 << 32, bytes_accessed=1 << 23, transcendentals=0),
        name="pick_pieces",
    )(live, donor, held)


def settle_body(alive, arrived, own, used, sem):
    def run(source):
        copy = pltpu.make_async_copy(source, used, sem)
        copy.start()
        copy.wait()

    @pl.when(alive[0] == 1)
    def _():
        run(own)

    @pl.when(alive[0] == 0)
    def _():
        run(arrived)


def settle(alive, arrived, own):
    return pl.pallas_call(
        settle_body,
        in_specs=[SMEM, FAR, FAR],
        out_specs=VMEM,
        out_shape=jax.ShapeDtypeStruct(own.shape, own.dtype),
        scratch_shapes=[pltpu.SemaphoreType.DMA],
        compiler_params=pltpu.CompilerParams(vmem_limit_bytes=SETTLE_LIMIT),
        cost_estimate=pl.CostEstimate(flops=1 << 31, bytes_accessed=1 << 22, transcendentals=0),
        name="settle_weights",
    )(alive, arrived, own)


def export_body(held, result, sem):
    copy = pltpu.make_async_copy(held, result, sem)
    copy.start()
    copy.wait()


def export(held):
    return pl.pallas_call(
        export_body,
        in_specs=[VMEM],
        out_specs=FAR,
        out_shape=jax.ShapeDtypeStruct(held.shape, held.dtype),
        scratch_shapes=[pltpu.SemaphoreType.DMA],
        compiler_params=pltpu.CompilerParams(vmem_limit_bytes=VMEM_LIMIT),
        name="export_rows",
    )(held)


def per_device(x_in, cotangent, norm_gain, w_up, w_down, live, donor):
    member = lax.axis_index("rep")
    level = lax.axis_index("section")
    depth = lax.axis_size("section")
    peers = lax.axis_size("rep")
    own_up = w_up[0, 0]
    own_down = w_down[0, 0]
    width, hidden_width = own_up.shape
    tokens = x_in.shape[1]
    m = tokens // MICRO

    def exchange(pieces):
        return lax.all_to_all(pieces, "rep", split_axis=0, concat_axis=0, tiled=True)

    alive = lax.dynamic_slice_in_dim(live, member, 1)

    def share(own):
        held = exchange(own.reshape(peers, -1, own.shape[1]))
        arrived = exchange(pick(held, live, donor))
        return settle(alive, arrived.reshape(own.shape), own)

    weights = (norm_gain, share(own_up), share(own_down))
    lags = [LAG_SLOW if s % 2 else LAG_FAST for s in range(depth - 1)]
    offsets = [sum(lags[:s]) for s in range(depth)]
    start = offsets[-1]
    back = [start + sum(lags[s:]) for s in range(depth)]
    forward = Relay(forward_body, "section_forward", x_in[0], offsets, 1, level, weights, m)
    backward = Relay(backward_body, "section_backward", cotangent[0], back, -1, level, weights, m)

    def shapes_of(*columns):
        return [(tokens, c) for c in columns]

    rows = normed = hidden = slope = outs = grads = pres = grads_in = None
    for turn in range(max(back) + MICRO):
        if forward.active(turn):
            rows, slope, normed, hidden, outs = forward.run(
                turn,
                [rows, slope, normed, hidden, outs],
                shapes_of(width, hidden_width, width, hidden_width, width),
            )
        if backward.active(turn):
            rows, slope, grads, pres, grads_in = backward.run(
                turn,
                [rows, slope, grads, pres, grads_in],
                shapes_of(width, hidden_width, width, hidden_width, width),
            )
    grad_up = mm(normed, pres, 0, 0).astype(jnp.bfloat16)
    grad_down = mm(hidden, grads, 0, 0).astype(jnp.bfloat16)
    return (export(outs)[None, None], export(grads_in)[None, None], grad_up[None, None], grad_down[None, None])


def solution(mesh):
    return jax.shard_map(
        per_device,
        mesh=mesh,
        in_specs=(
            P("rep", None, None),
            P("rep", None, None),
            P("section", None),
            P("rep", "section", None, None),
            P("rep", "section", None, None),
            P(),
            P(),
        ),
        out_specs=(
            P("rep", "section", None, None),
            P("rep", "section", None, None),
            P("rep", "section", None, None),
            P("rep", "section", None, None),
        ),
        check_vma=False,
    )
```

```python
import functools

import jax
import jax.numpy as jnp
from jax import lax
from jax.experimental import pallas as pl
from jax.experimental.pallas import tpu as pltpu
from jax.sharding import PartitionSpec as P

MICRO = 3
CHUNK = 512
PARTS = 4
FINISH_LIMIT = 36 * 1024 * 1024
LAG_FAST = 1
LAG_SLOW = 2
GELU_C = 0.7978845608028654
CUBIC = 0.044715
VMEM_LIMIT = 16 * 1024 * 1024
COPY_LIMIT = 62 * 1024 * 1024
SETTLE_LIMIT = 44 * 1024 * 1024
VMEM = pl.BlockSpec(memory_space=pltpu.VMEM)
SMEM = pl.BlockSpec(memory_space=pltpu.SMEM)
FAR = pl.BlockSpec(memory_space=pl.ANY)


def row_stats(values):
    center = values - jnp.mean(values, axis=-1, keepdims=True)
    factor = lax.rsqrt(jnp.mean(center * center, axis=-1, keepdims=True) + 1e-05)
    return center * factor, factor


def mm(left, right, left_dim, right_dim):
    return lax.dot_general(
        left, right, (((left_dim,), (right_dim,)), ((), ())), preferred_element_type=jnp.float32
    )


def gelu_and_slope(u):
    square = u * u
    half = 0.5 + 0.5 * jnp.tanh(u * (GELU_C + (GELU_C * CUBIC) * square))
    slope = half + (half - half * half) * (
        u * (2.0 * GELU_C + (6.0 * GELU_C * CUBIC) * square)
    )
    return u * half, slope


def choose(level, place, sources):
    def read(kind, ref):
        return ref[place, :] if kind == "slot" else ref[...]

    value = read(*sources[-1][1:])
    for levels, kind, ref in sources[:-1]:
        hit = functools.reduce(jnp.logical_or, [level == k for k in levels])
        value = jnp.where(hit, read(kind, ref), value)
    return value


def forward_body(heads, n_held, m, meta, *refs):
    sources = [(*head, ref) for head, ref in zip(heads, refs)]
    gain, up, down = refs[len(heads) : len(heads) + 3]
    send, rows_o, slope_o, normed_o, hidden_o, out_o = refs[len(heads) + 3 + n_held :]
    place = pl.ds(pl.multiple_of(meta[0] * m, m), m)

    @pl.when(meta[1] == 1)
    def _():
        rows = choose(meta[2], place, sources)
        rows_o[place, :] = rows
        xhat, _ = row_stats(rows.astype(jnp.float32))
        normed = (xhat * gain[...]).astype(jnp.bfloat16)
        normed_o[place, :] = normed
        for j in range(up.shape[1] // CHUNK):
            cut = slice(j * CHUNK, (j + 1) * CHUNK)
            hidden, slope = gelu_and_slope(mm(normed, up[:, cut], 1, 0))
            hidden_o[place, cut] = hidden.astype(jnp.bfloat16)
            slope_o[place, cut] = slope.astype(jnp.bfloat16)
        for j in range(down.shape[1] // CHUNK):
            cut = slice(j * CHUNK, (j + 1) * CHUNK)
            total = rows_o[place, cut].astype(jnp.float32) + mm(
                hidden_o[place, :], down[:, cut], 1, 0
            )
            send[:, cut] = total.astype(jnp.bfloat16)
            out_o[place, cut] = send[:, cut]


def backward_body(heads, n_held, m, meta, *refs):
    sources = [(*head, ref) for head, ref in zip(heads, refs)]
    gain, up, down = refs[len(heads) : len(heads) + 3]
    send, rows_i, slope_i, grad_o, pre_o, grad_in_o = refs[len(heads) + 3 + n_held :]
    place = pl.ds(pl.multiple_of(meta[0] * m, m), m)

    @pl.when(meta[1] == 1)
    def _():
        grad = choose(meta[2], place, sources)
        grad_o[place, :] = grad
        for j in range(up.shape[1] // CHUNK):
            cut = slice(j * CHUNK, (j + 1) * CHUNK)
            grad_hidden = mm(grad, down[cut, :], 1, 1)
            pre_o[place, cut] = (grad_hidden * slope_i[place, cut].astype(jnp.float32)).astype(
                jnp.bfloat16
            )
        q = mm(pre_o[place, :], up[...], 1, 1) * gain[...]
        xhat, factor = row_stats(rows_i[place, :].astype(jnp.float32))
        centered = (
            q
            - jnp.mean(q, axis=-1, keepdims=True)
            - xhat * jnp.mean(q * xhat, axis=-1, keepdims=True)
        )
        result = (grad.astype(jnp.float32) + factor * centered).astype(jnp.bfloat16)
        send[...] = result
        grad_in_o[place, :] = result


def stage(body, name, meta, sources, weights, held, shapes, m):
    width, hidden = weights[1].shape
    given = [i for i, a in enumerate(held) if a is not None]
    operands = [a for _, _, a in sources] + list(weights)
    n_before = len(operands)
    operands += [held[i] for i in given]
    result = pl.pallas_call(
        functools.partial(body, [s[:2] for s in sources], len(given), m),
        in_specs=[SMEM] + [VMEM] * n_before + [VMEM] * len(given),
        out_specs=[VMEM] * (1 + len(shapes)),
        out_shape=[jax.ShapeDtypeStruct(s, jnp.bfloat16) for s in [(m, width)] + shapes],
        input_output_aliases={1 + n_before + k: 1 + i for k, i in enumerate(given)},
        compiler_params=pltpu.CompilerParams(vmem_limit_bytes=VMEM_LIMIT),
        cost_estimate=pl.CostEstimate(
            flops=4 * m * width * hidden, bytes_accessed=4 * width * hidden, transcendentals=0
        ),
        name=name,
    )(meta, *operands)
    return result[0], list(result[1:])


class Relay:
    def __init__(self, body, name, entry, offsets, direction, level, weights, m):
        self.body, self.name, self.entry = body, name, entry
        self.offsets, self.direction, self.level = offsets, direction, level
        self.weights, self.m = weights, m
        self.arrays = {}

    def active(self, turn):
        return [s for s, o in enumerate(self.offsets) if 0 <= turn - o < MICRO]

    def run(self, turn, held, shapes):
        offsets, direction = self.offsets, self.direction
        depth = len(offsets)
        head = 0 if direction > 0 else depth - 1
        active = self.active(turn)
        index = turn - jnp.asarray(offsets, jnp.int32)[self.level]
        valid = (index >= 0) & (index < MICRO)
        slot = jnp.clip(index, 0, MICRO - 1)
        meta = jnp.stack([slot, valid.astype(jnp.int32), self.level]).astype(jnp.int32)
        by_array = {}
        for s in active:
            lag = None if s == head else offsets[s] - offsets[s - direction]
            by_array.setdefault(lag, []).append(s)
        sources = [
            (levels, "slot", self.entry)
            if lag is None
            else (levels, "whole", self.arrays[turn - lag, lag])
            for lag, levels in by_array.items()
        ]
        send, held = stage(
            self.body, self.name, meta, sources, self.weights, held, shapes, self.m
        )
        groups = {}
        for s in active:
            if 0 <= s + direction < depth:
                groups.setdefault(offsets[s + direction] - offsets[s], []).append(s)
        for lag, members in groups.items():
            pairs = [(s, s + direction) for s in members]
            self.arrays[turn, lag] = lax.ppermute(send, "section", pairs)
        return held


def pick_body(live, donor, held, picked, room, in_sems, out_sems):
    def load(j):
        return pltpu.make_async_copy(held.at[donor[j]], room.at[j], in_sems.at[j])

    def save(j):
        return pltpu.make_async_copy(room.at[j], picked.at[j], out_sems.at[j])

    def each(action):
        def step(j, carry):
            @pl.when(live[j] == 0)
            def _():
                action(j)

            return carry

        lax.fori_loop(0, held.shape[0], step, 0)

    def pass_on(j):
        load(j).wait()
        save(j).start()

    each(lambda j: load(j).start())
    each(pass_on)
    each(lambda j: save(j).wait())


def pick(held, live, donor):
    peers = held.shape[0]
    return pl.pallas_call(
        pick_body,
        in_specs=[SMEM, SMEM, FAR],
        out_specs=FAR,
        out_shape=jax.ShapeDtypeStruct(held.shape, held.dtype),
        scratch_shapes=[
            pltpu.VMEM(held.shape, held.dtype),
            pltpu.SemaphoreType.DMA((peers,)),
            pltpu.SemaphoreType.DMA((peers,)),
        ],
        compiler_params=pltpu.CompilerParams(vmem_limit_bytes=COPY_LIMIT),
        cost_estimate=pl.CostEstimate(flops=1 << 32, bytes_accessed=1 << 23, transcendentals=0),
        name="pick_pieces",
    )(live, donor, held)


def settle_body(alive, arrived, own, used, sem):
    def run(source):
        copy = pltpu.make_async_copy(source, used, sem)
        copy.start()
        copy.wait()

    @pl.when(alive[0] == 1)
    def _():
        run(own)

    @pl.when(alive[0] == 0)
    def _():
        run(arrived)


def settle(alive, arrived, own):
    return pl.pallas_call(
        settle_body,
        in_specs=[SMEM, FAR, FAR],
        out_specs=VMEM,
        out_shape=jax.ShapeDtypeStruct(own.shape, own.dtype),
        scratch_shapes=[pltpu.SemaphoreType.DMA],
        compiler_params=pltpu.CompilerParams(vmem_limit_bytes=SETTLE_LIMIT),
        cost_estimate=pl.CostEstimate(flops=1 << 31, bytes_accessed=1 << 22, transcendentals=0),
        name="settle_weights",
    )(alive, arrived, own)


def finish_body(normed, pres, hidden, grads, outs, grads_in, *refs):
    up_o, down_o, outs_o, grads_in_o, up_s, down_s, up_sems, down_sems, row_sems = refs
    row_copies = [
        pltpu.make_async_copy(outs, outs_o, row_sems.at[0]),
        pltpu.make_async_copy(grads_in, grads_in_o, row_sems.at[1]),
    ]
    for copy in row_copies:
        copy.start()

    def part(left, right, held, result, sems, i):
        rows = held.shape[0] // PARTS
        cut = pl.ds(pl.multiple_of(i * rows, rows), rows)
        return cut, pltpu.make_async_copy(held.at[cut, :], result.at[cut, :], sems.at[i])

    jobs = [
        (normed, pres, up_s, up_o, up_sems),
        (hidden, grads, down_s, down_o, down_sems),
    ]
    for job in jobs:
        left, right, held = job[:3]

        def step(i, carry, job=job, left=left, right=right, held=held):
            cut, copy = part(*job, i)
            held[cut, :] = mm(left[:, cut], right[...], 0, 0).astype(held.dtype)
            copy.start()
            return carry

        lax.fori_loop(0, PARTS, step, 0)
    for job in jobs:
        for i in range(PARTS):
            part(*job, i)[1].wait()
    for copy in row_copies:
        copy.wait()


def finish(normed, pres, hidden, grads, outs, grads_in):
    width, hidden_width = normed.shape[1], hidden.shape[1]
    shapes = [(width, hidden_width), (hidden_width, width), outs.shape, grads_in.shape]
    return pl.pallas_call(
        finish_body,
        in_specs=[VMEM] * 6,
        out_specs=[FAR] * 4,
        out_shape=[jax.ShapeDtypeStruct(s, jnp.bfloat16) for s in shapes],
        scratch_shapes=[
            pltpu.VMEM(shapes[0], jnp.bfloat16),
            pltpu.VMEM(shapes[1], jnp.bfloat16),
            pltpu.SemaphoreType.DMA((PARTS,)),
            pltpu.SemaphoreType.DMA((PARTS,)),
            pltpu.SemaphoreType.DMA((2,)),
        ],
        compiler_params=pltpu.CompilerParams(vmem_limit_bytes=FINISH_LIMIT),
        name="weight_gradients",
    )(normed, pres, hidden, grads, outs, grads_in)


def per_device(x_in, cotangent, norm_gain, w_up, w_down, live, donor):
    member = lax.axis_index("rep")
    level = lax.axis_index("section")
    depth = lax.axis_size("section")
    peers = lax.axis_size("rep")
    own_up = w_up[0, 0]
    own_down = w_down[0, 0]
    width, hidden_width = own_up.shape
    tokens = x_in.shape[1]
    m = tokens // MICRO

    def exchange(pieces):
        return lax.all_to_all(pieces, "rep", split_axis=0, concat_axis=0, tiled=True)

    alive = lax.dynamic_slice_in_dim(live, member, 1)

    def share(own):
        held = exchange(own.reshape(peers, -1, own.shape[1]))
        arrived = exchange(pick(held, live, donor))
        return settle(alive, arrived.reshape(own.shape), own)

    weights = (norm_gain, share(own_up), share(own_down))
    lags = [LAG_SLOW if s % 2 else LAG_FAST for s in range(depth - 1)]
    offsets = [sum(lags[:s]) for s in range(depth)]
    start = offsets[-1]
    back = [start + sum(lags[s:]) for s in range(depth)]
    forward = Relay(forward_body, "section_forward", x_in[0], offsets, 1, level, weights, m)
    backward = Relay(backward_body, "section_backward", cotangent[0], back, -1, level, weights, m)

    def shapes_of(*columns):
        return [(tokens, c) for c in columns]

    rows = normed = hidden = slope = outs = grads = pres = grads_in = None
    for turn in range(max(back) + MICRO):
        if forward.active(turn):
            rows, slope, normed, hidden, outs = forward.run(
                turn,
                [rows, slope, normed, hidden, outs],
                shapes_of(width, hidden_width, width, hidden_width, width),
            )
        if backward.active(turn):
            rows, slope, grads, pres, grads_in = backward.run(
                turn,
                [rows, slope, grads, pres, grads_in],
                shapes_of(width, hidden_width, width, hidden_width, width),
            )
    grad_up, grad_down, section_out, section_in_grad = finish(
        normed, pres, hidden, grads, outs, grads_in
    )
    return (
        section_out[None, None],
        section_in_grad[None, None],
        grad_up[None, None],
        grad_down[None, None],
    )


def solution(mesh):
    return jax.shard_map(
        per_device,
        mesh=mesh,
        in_specs=(
            P("rep", None, None),
            P("rep", None, None),
            P("section", None),
            P("rep", "section", None, None),
            P("rep", "section", None, None),
            P(),
            P(),
        ),
        out_specs=(
            P("rep", "section", None, None),
            P("rep", "section", None, None),
            P("rep", "section", None, None),
            P("rep", "section", None, None),
        ),
        check_vma=False,
    )
```

```python
import functools

import jax
import jax.numpy as jnp
from jax import lax
from jax.experimental import pallas as pl
from jax.experimental.pallas import tpu as pltpu
from jax.sharding import PartitionSpec as P

MICRO = 3
CHUNK = 256
PARTS = 2
FINISH_LIMIT = 36 * 1024 * 1024
LAG_FAST = 1
LAG_SLOW = 2
GELU_C = 0.7978845608028654
CUBIC = 0.044715
VMEM_LIMIT = 16 * 1024 * 1024
COPY_LIMIT = 62 * 1024 * 1024
SETTLE_LIMIT = 44 * 1024 * 1024
VMEM = pl.BlockSpec(memory_space=pltpu.VMEM)
SMEM = pl.BlockSpec(memory_space=pltpu.SMEM)
FAR = pl.BlockSpec(memory_space=pl.ANY)


def row_stats(values):
    center = values - jnp.mean(values, axis=-1, keepdims=True)
    factor = lax.rsqrt(jnp.mean(center * center, axis=-1, keepdims=True) + 1e-05)
    return center * factor, factor


def mm(left, right, left_dim, right_dim):
    return lax.dot_general(
        left, right, (((left_dim,), (right_dim,)), ((), ())), preferred_element_type=jnp.float32
    )


def gelu_and_slope(u):
    square = u * u
    half = 0.5 + 0.5 * jnp.tanh(u * (GELU_C + (GELU_C * CUBIC) * square))
    slope = half + (half - half * half) * (
        u * (2.0 * GELU_C + (6.0 * GELU_C * CUBIC) * square)
    )
    return u * half, slope


def choose(level, place, sources):
    def read(kind, ref):
        return ref[place, :] if kind == "slot" else ref[...]

    value = read(*sources[-1][1:])
    for levels, kind, ref in sources[:-1]:
        hit = functools.reduce(jnp.logical_or, [level == k for k in levels])
        value = jnp.where(hit, read(kind, ref), value)
    return value


def forward_body(heads, n_held, m, meta, *refs):
    sources = [(*head, ref) for head, ref in zip(heads, refs)]
    gain, up, down = refs[len(heads) : len(heads) + 3]
    send, rows_o, slope_o, normed_o, hidden_o, out_o = refs[len(heads) + 3 + n_held :]
    place = pl.ds(pl.multiple_of(meta[0] * m, m), m)

    @pl.when(meta[1] == 1)
    def _():
        rows = choose(meta[2], place, sources)
        rows_o[place, :] = rows
        xhat, _ = row_stats(rows.astype(jnp.float32))
        normed = (xhat * gain[...]).astype(jnp.bfloat16)
        normed_o[place, :] = normed
        for j in range(up.shape[1] // CHUNK):
            cut = slice(j * CHUNK, (j + 1) * CHUNK)
            hidden, slope = gelu_and_slope(mm(normed, up[:, cut], 1, 0))
            hidden_o[place, cut] = hidden.astype(jnp.bfloat16)
            slope_o[place, cut] = slope.astype(jnp.bfloat16)
        for j in range(down.shape[1] // CHUNK):
            cut = slice(j * CHUNK, (j + 1) * CHUNK)
            total = rows_o[place, cut].astype(jnp.float32) + mm(
                hidden_o[place, :], down[:, cut], 1, 0
            )
            send[:, cut] = total.astype(jnp.bfloat16)
            out_o[place, cut] = send[:, cut]


def backward_body(heads, n_held, m, meta, *refs):
    sources = [(*head, ref) for head, ref in zip(heads, refs)]
    gain, up, down = refs[len(heads) : len(heads) + 3]
    send, rows_i, slope_i, grad_o, pre_o, grad_in_o = refs[len(heads) + 3 + n_held :]
    place = pl.ds(pl.multiple_of(meta[0] * m, m), m)

    @pl.when(meta[1] == 1)
    def _():
        grad = choose(meta[2], place, sources)
        grad_o[place, :] = grad
        for j in range(up.shape[1] // CHUNK):
            cut = slice(j * CHUNK, (j + 1) * CHUNK)
            grad_hidden = mm(grad, down[cut, :], 1, 1)
            pre_o[place, cut] = (grad_hidden * slope_i[place, cut].astype(jnp.float32)).astype(
                jnp.bfloat16
            )
        q = mm(pre_o[place, :], up[...], 1, 1) * gain[...]
        xhat, factor = row_stats(rows_i[place, :].astype(jnp.float32))
        centered = (
            q
            - jnp.mean(q, axis=-1, keepdims=True)
            - xhat * jnp.mean(q * xhat, axis=-1, keepdims=True)
        )
        result = (grad.astype(jnp.float32) + factor * centered).astype(jnp.bfloat16)
        send[...] = result
        grad_in_o[place, :] = result


def unsent(body, heads, n_held, m, meta, *refs):
    n_in = len(heads) + 3 + n_held
    body(heads, n_held, m, meta, *refs[:n_in], refs[-1], *refs[n_in:-1])


def stage(body, name, meta, sources, weights, held, shapes, m, sends):
    width, hidden = weights[1].shape
    given = [i for i, a in enumerate(held) if a is not None]
    operands = [a for _, _, a in sources] + list(weights)
    n_before = len(operands)
    operands += [held[i] for i in given]
    message = (m, width)
    first = [message] if sends else []
    result = pl.pallas_call(
        functools.partial(
            body if sends else functools.partial(unsent, body),
            [s[:2] for s in sources],
            len(given),
            m,
        ),
        in_specs=[SMEM] + [VMEM] * len(operands),
        out_specs=[VMEM] * len(first + shapes),
        out_shape=[jax.ShapeDtypeStruct(s, jnp.bfloat16) for s in first + shapes],
        scratch_shapes=[] if sends else [pltpu.VMEM(message, jnp.bfloat16)],
        input_output_aliases={1 + n_before + k: len(first) + i for k, i in enumerate(given)},
        compiler_params=pltpu.CompilerParams(vmem_limit_bytes=VMEM_LIMIT),
        cost_estimate=pl.CostEstimate(
            flops=4 * m * width * hidden, bytes_accessed=4 * width * hidden, transcendentals=0
        ),
        name=name,
    )(meta, *operands)
    return (result[0] if sends else None), list(result[len(first) :])


class Relay:
    def __init__(self, body, name, entry, offsets, direction, level, weights, m):
        self.body, self.name, self.entry = body, name, entry
        self.offsets, self.direction, self.level = offsets, direction, level
        self.weights, self.m = weights, m
        self.arrays = {}

    def active(self, turn):
        return [s for s, o in enumerate(self.offsets) if 0 <= turn - o < MICRO]

    def run(self, turn, held, shapes):
        offsets, direction = self.offsets, self.direction
        depth = len(offsets)
        head = 0 if direction > 0 else depth - 1
        active = self.active(turn)
        index = turn - jnp.asarray(offsets, jnp.int32)[self.level]
        valid = (index >= 0) & (index < MICRO)
        slot = jnp.clip(index, 0, MICRO - 1)
        meta = jnp.stack([slot, valid.astype(jnp.int32), self.level]).astype(jnp.int32)
        by_array = {}
        for s in active:
            lag = None if s == head else offsets[s] - offsets[s - direction]
            by_array.setdefault(lag, []).append(s)
        sources = [
            (levels, "slot", self.entry)
            if lag is None
            else (levels, "whole", self.arrays[turn - lag, lag])
            for lag, levels in by_array.items()
        ]
        send, held = stage(
            self.body, self.name, meta, sources, self.weights, held, shapes, self.m,
            any(0 <= s + direction < depth for s in active),
        )
        groups = {}
        for s in active:
            if 0 <= s + direction < depth:
                groups.setdefault(offsets[s + direction] - offsets[s], []).append(s)
        for lag, members in groups.items():
            pairs = [(s, s + direction) for s in members]
            self.arrays[turn, lag] = lax.ppermute(send, "section", pairs)
        return held


def pick_body(live, donor, held, picked, room, in_sems, out_sems):
    def load(j):
        return pltpu.make_async_copy(held.at[donor[j]], room.at[j], in_sems.at[j])

    def save(j):
        return pltpu.make_async_copy(room.at[j], picked.at[j], out_sems.at[j])

    def each(action):
        def step(j, carry):
            @pl.when(live[j] == 0)
            def _():
                action(j)

            return carry

        lax.fori_loop(0, held.shape[0], step, 0)

    def pass_on(j):
        load(j).wait()
        save(j).start()

    each(lambda j: load(j).start())
    each(pass_on)
    each(lambda j: save(j).wait())


def pick(held, live, donor):
    peers = held.shape[0]
    return pl.pallas_call(
        pick_body,
        in_specs=[SMEM, SMEM, FAR],
        out_specs=FAR,
        out_shape=jax.ShapeDtypeStruct(held.shape, held.dtype),
        scratch_shapes=[
            pltpu.VMEM(held.shape, held.dtype),
            pltpu.SemaphoreType.DMA((peers,)),
            pltpu.SemaphoreType.DMA((peers,)),
        ],
        compiler_params=pltpu.CompilerParams(vmem_limit_bytes=COPY_LIMIT),
        cost_estimate=pl.CostEstimate(flops=1 << 32, bytes_accessed=1 << 23, transcendentals=0),
        name="pick_pieces",
    )(live, donor, held)


def settle_body(alive, arrived, own, used, sem):
    def run(source):
        copy = pltpu.make_async_copy(source, used, sem)
        copy.start()
        copy.wait()

    @pl.when(alive[0] == 1)
    def _():
        run(own)

    @pl.when(alive[0] == 0)
    def _():
        run(arrived)


def settle(alive, arrived, own):
    return pl.pallas_call(
        settle_body,
        in_specs=[SMEM, FAR, FAR],
        out_specs=VMEM,
        out_shape=jax.ShapeDtypeStruct(own.shape, own.dtype),
        scratch_shapes=[pltpu.SemaphoreType.DMA],
        compiler_params=pltpu.CompilerParams(vmem_limit_bytes=SETTLE_LIMIT),
        cost_estimate=pl.CostEstimate(flops=1 << 31, bytes_accessed=1 << 22, transcendentals=0),
        name="settle_weights",
    )(alive, arrived, own)


def finish_body(normed, pres, hidden, grads, outs, grads_in, *refs):
    up_o, down_o, outs_o, grads_in_o, up_s, down_s, up_sems, down_sems, row_sems = refs
    row_copies = [
        pltpu.make_async_copy(outs, outs_o, row_sems.at[0]),
        pltpu.make_async_copy(grads_in, grads_in_o, row_sems.at[1]),
    ]
    for copy in row_copies:
        copy.start()

    def part(left, right, held, result, sems, i):
        rows = held.shape[0] // PARTS
        cut = pl.ds(pl.multiple_of(i * rows, rows), rows)
        return cut, pltpu.make_async_copy(held.at[cut, :], result.at[cut, :], sems.at[i])

    jobs = [
        (normed, pres, up_s, up_o, up_sems),
        (hidden, grads, down_s, down_o, down_sems),
    ]
    for job in jobs:
        left, right, held = job[:3]

        def step(i, carry, job=job, left=left, right=right, held=held):
            cut, copy = part(*job, i)
            held[cut, :] = mm(left[:, cut], right[...], 0, 0).astype(held.dtype)
            copy.start()
            return carry

        lax.fori_loop(0, PARTS, step, 0)
    for job in jobs:
        for i in range(PARTS):
            part(*job, i)[1].wait()
    for copy in row_copies:
        copy.wait()


def finish(normed, pres, hidden, grads, outs, grads_in):
    width, hidden_width = normed.shape[1], hidden.shape[1]
    shapes = [(width, hidden_width), (hidden_width, width), outs.shape, grads_in.shape]
    return pl.pallas_call(
        finish_body,
        in_specs=[VMEM] * 6,
        out_specs=[FAR] * 4,
        out_shape=[jax.ShapeDtypeStruct(s, jnp.bfloat16) for s in shapes],
        scratch_shapes=[
            pltpu.VMEM(shapes[0], jnp.bfloat16),
            pltpu.VMEM(shapes[1], jnp.bfloat16),
            pltpu.SemaphoreType.DMA((PARTS,)),
            pltpu.SemaphoreType.DMA((PARTS,)),
            pltpu.SemaphoreType.DMA((2,)),
        ],
        compiler_params=pltpu.CompilerParams(vmem_limit_bytes=FINISH_LIMIT),
        name="weight_gradients",
    )(normed, pres, hidden, grads, outs, grads_in)


def per_device(x_in, cotangent, norm_gain, w_up, w_down, live, donor):
    member = lax.axis_index("rep")
    level = lax.axis_index("section")
    depth = lax.axis_size("section")
    peers = lax.axis_size("rep")
    own_up = w_up[0, 0]
    own_down = w_down[0, 0]
    width, hidden_width = own_up.shape
    tokens = x_in.shape[1]
    m = tokens // MICRO

    def exchange(pieces):
        return lax.all_to_all(pieces, "rep", split_axis=0, concat_axis=0, tiled=True)

    alive = lax.dynamic_slice_in_dim(live, member, 1)

    def share(own):
        held = exchange(own.reshape(peers, -1, own.shape[1]))
        arrived = exchange(pick(held, live, donor))
        return settle(alive, arrived.reshape(own.shape), own)

    weights = (norm_gain, share(own_up), share(own_down))
    lags = [LAG_SLOW if s % 2 else LAG_FAST for s in range(depth - 1)]
    offsets = [sum(lags[:s]) for s in range(depth)]
    start = offsets[-1]
    back = [start + sum(lags[s:]) for s in range(depth)]
    forward = Relay(forward_body, "section_forward", x_in[0], offsets, 1, level, weights, m)
    backward = Relay(backward_body, "section_backward", cotangent[0], back, -1, level, weights, m)

    def shapes_of(*columns):
        return [(tokens, c) for c in columns]

    rows = normed = hidden = slope = outs = grads = pres = grads_in = None
    for turn in range(max(back) + MICRO):
        if forward.active(turn):
            rows, slope, normed, hidden, outs = forward.run(
                turn,
                [rows, slope, normed, hidden, outs],
                shapes_of(width, hidden_width, width, hidden_width, width),
            )
        if backward.active(turn):
            rows, slope, grads, pres, grads_in = backward.run(
                turn,
                [rows, slope, grads, pres, grads_in],
                shapes_of(width, hidden_width, width, hidden_width, width),
            )
    grad_up, grad_down, section_out, section_in_grad = finish(
        normed, pres, hidden, grads, outs, grads_in
    )
    return (
        section_out[None, None],
        section_in_grad[None, None],
        grad_up[None, None],
        grad_down[None, None],
    )


def solution(mesh):
    return jax.shard_map(
        per_device,
        mesh=mesh,
        in_specs=(
            P("rep", None, None),
            P("rep", None, None),
            P("section", None),
            P("rep", "section", None, None),
            P("rep", "section", None, None),
            P(),
            P(),
        ),
        out_specs=(
            P("rep", "section", None, None),
            P("rep", "section", None, None),
            P("rep", "section", None, None),
            P("rep", "section", None, None),
        ),
        check_vma=False,
    )
```
